16 devices in a mesh: rep: 4 (over y, z, core), dp: 4 (over x).
Axes of the slice: x: 4, y: 2, z: 1, core: 2. Of those that a mesh axis runs over, the one named last changes fastest.
The devices are a block of a 4x4x8 slice.
Arguments:
- x: bfloat16 [16, 1024, 1024], P(('rep', 'dp')), parts along dimension 0
- dy: bfloat16 [16, 1024, 1024], P(('rep', 'dp')), parts along dimension 0
- w_gate: bfloat16 [2, 1024, 3200], replicated
- w_up: bfloat16 [2, 1024, 3200], replicated
- w_down: bfloat16 [2, 3200, 1024], replicated
- m_w_gate: float32 [2, 1024, 3200], replicated
- m_w_up: float32 [2, 1024, 3200], replicated
- m_w_down: float32 [2, 3200, 1024], replicated
- v_w_gate: float32 [2, 1024, 3200], replicated
- v_w_up: float32 [2, 1024, 3200], replicated
- v_w_down: float32 [2, 3200, 1024], replicated
Outputs:
- output 1: bfloat16 [8, 1024, 3200], P('rep'), parts along dimension 0
- output 2: bfloat16 [8, 1024, 3200], P('rep'), parts along dimension 0
- output 3: bfloat16 [8, 3200, 1024], P('rep'), parts along dimension 0
- output 4: float32 [8, 1024, 3200], P('rep'), parts along dimension 0
- output 5: float32 [8, 1024, 3200], P('rep'), parts along dimension 0
- output 6: float32 [8, 3200, 1024], P('rep'), parts along dimension 0
- output 7: float32 [8, 1024, 3200], P('rep'), parts along dimension 0
- output 8: float32 [8, 1024, 3200], P('rep'), parts along dimension 0
- output 9: float32 [8, 3200, 1024], P('rep'), parts along dimension 0
There are 4 independent parts. The reference program is written for one: setup_inputs(seed, part) draws one part's arguments, and reference() takes and returns one part's arrays. A program takes and returns all parts, laid end to end along the dimension named above; an argument that names none is the same for every part.
All inputs are finite; a program needn't handle non-finite values.
Results may differ from the reference program's by a relative error of at most 0.022.
Values are sent between devices in bfloat16 or wider.
A program may use at most 768 MiB of HBM per device.

```python
import jax
import jax.numpy as jnp
from jax import lax

SEQUENCES = 4
TOKENS = 1024
D = 1024
FF = 3200
LAYERS = 2
NAMES = ("w_gate", "w_up", "w_down")
SHAPES = {"w_gate": (LAYERS, D, FF), "w_up": (LAYERS, D, FF), "w_down": (LAYERS, FF, D)}


def bump(key, n, height):
    away = (jnp.arange(n, dtype=jnp.int32) - jax.random.randint(key, (), 0, n, jnp.int32)) % n
    return jnp.where(away < n // 8, height, 1.0)


def together(key, own, strength):
    shared = jax.random.normal(key, own.shape[1:], jnp.float32)
    return (own + strength * shared) * lax.rsqrt(1 + strength * strength)


def setup_inputs(seed: int = 0, part: int = 0) -> dict:
    kx, kdy, ka, kb, kz, kf, kh, kl, *keys = jax.random.split(jax.random.key(seed), 8 + 3 * len(NAMES))
    kx, kdy, ka, kb = (jax.random.fold_in(k, part) for k in (kx, kdy, ka, kb))
    kw, km, kv = (keys[i::3] for i in range(3))
    shape = (SEQUENCES, TOKENS, D)
    much_x, much_dy = jax.random.uniform(kz, (2,), jnp.float32, 0.0, 1.0)
    loud = 2.0 ** jax.random.uniform(jax.random.fold_in(kz, 1), (), jnp.float32, -1.0, 2.0)
    layers = 2.0 ** jax.random.uniform(kl, (LAYERS, 1, 1), jnp.float32, -1.0, 1.0)
    x = together(ka, jax.random.normal(kx, shape, jnp.float32), much_x) * bump(kf, D, 4.0)
    dy = together(kb, jax.random.normal(kdy, shape, jnp.float32), much_dy)
    drawn = {"x": x.astype(jnp.bfloat16), "dy": (loud * dy * (SEQUENCES * TOKENS) ** -0.5).astype(jnp.bfloat16)}
    for key, name in zip(kw, NAMES, strict=True):
        w = jax.random.normal(key, SHAPES[name], jnp.float32) * SHAPES[name][1] ** -0.5
        drawn[name] = (w * {"w_gate": 1.0, "w_up": bump(kh, FF, 4.0), "w_down": layers}[name]).astype(jnp.bfloat16)
    for key, name in zip(km, NAMES, strict=True):
        drawn[f"m_{name}"] = 0.1 * jax.random.normal(key, SHAPES[name], jnp.float32)
    for key, name in zip(kv, NAMES, strict=True):
        drawn[f"v_{name}"] = jax.random.uniform(key, SHAPES[name], jnp.float32, 0.005, 0.015)
    return drawn


def matmul(a, w):
    return jnp.dot(a, w, preferred_element_type=jnp.float32).astype(jnp.bfloat16)


def normed(h):
    wide = h.astype(jnp.float32)
    scale = lax.rsqrt(jnp.mean(wide**2, -1, keepdims=True) + 1e-6)
    return (wide * scale).astype(jnp.bfloat16)


def layer(h, w):
    a = normed(h)
    gate = jnp.dot(a, w["w_gate"], preferred_element_type=jnp.float32)
    up = jnp.dot(a, w["w_up"], preferred_element_type=jnp.float32)
    return h + matmul((jax.nn.silu(gate) * up).astype(jnp.bfloat16), w["w_down"])


def adamw(w, m, v, g):
    m = 0.9 * m + 0.1 * g
    v = 0.95 * v + 0.05 * g * g
    step = m * lax.rsqrt(v + 1e-8) + 0.1 * w
    return (w - 0.02 * step).astype(jnp.bfloat16), m, v


def clipped(gradients, sum_of_squares, count):
    factor = jnp.minimum(1.0, 0.5 * lax.rsqrt(sum_of_squares / count + 1e-30))
    return [g * factor for g in gradients]


def stack(weights, h):
    return lax.scan(lambda h, w: (layer(h, w), None), h, weights)[0]


def reference(x, dy, w_gate, w_up, w_down, m_w_gate, m_w_up, m_w_down, v_w_gate, v_w_up, v_w_down):
    weights = dict(zip(NAMES, (w_gate, w_up, w_down), strict=True))

    def take(so_far, sequence):
        h, by_y = sequence
        _, back = jax.vjp(lambda w: stack(w, h), weights)
        return jax.tree.map(lambda total, term: total + term.astype(jnp.float32), so_far, back(by_y)[0]), None

    none_yet = {name: jnp.zeros(w.shape, jnp.float32) for name, w in weights.items()}
    by_weights, _ = lax.scan(take, none_yet, (x, dy))
    gradients = [by_weights[name].astype(jnp.bfloat16).astype(jnp.float32) for name in NAMES]
    gradients = clipped(gradients, sum(jnp.sum(g * g) for g in gradients), sum(g.size for g in gradients))
    new = [
        adamw(w.astype(jnp.float32), m, v, g)
        for w, m, v, g in zip((w_gate, w_up, w_down), (m_w_gate, m_w_up, m_w_down), (v_w_gate, v_w_up, v_w_down), gradients, strict=True)
    ]
    return tuple(one[which] for which in range(3) for one in new)
```

```python
import functools

import jax
import jax.numpy as jnp
from jax import lax
from jax.experimental import pallas as pl
from jax.experimental.pallas import tpu as pltpu
from jax.sharding import PartitionSpec as P

F32, BF16 = jnp.float32, jnp.bfloat16
LANES = 128
STEPS = 8


def normed(h):
    wide = h.astype(F32)
    scale = lax.rsqrt(jnp.mean(wide**2, -1, keepdims=True) + 1e-6)
    return (wide * scale).astype(BF16)


def dot(a, b, da=1, db=0):
    return lax.dot_general(a, b, (((da,), (db,)), ((), ())), preferred_element_type=F32)


def gated(a, dout, w_gate, w_up, w_down):
    gate, up = dot(a, w_gate), dot(a, w_up)
    by_hidden = dot(dout, w_down, 1, 1).astype(BF16).astype(F32)
    s = jax.nn.sigmoid(gate)
    silu = gate * s
    hidden = (silu * up).astype(BF16)
    by_up = (by_hidden * silu).astype(BF16)
    by_gate = (by_hidden * up * (s * (1 + gate * (1 - s)))).astype(BF16)
    return hidden, by_gate, by_up


def adamw_kernel(at, factor, *refs):
    del at
    grads, w, m, v = (refs[i : i + 3] for i in (0, 3, 6, 9))
    w_out, m_out, v_out = (refs[len(refs) - 9 + i : len(refs) - 6 + i] for i in (0, 3, 6))
    c = factor[0]
    for i in range(3):
        g = grads[i][...].astype(F32) * c
        mm = 0.9 * m[i][0] + 0.1 * g
        vv = 0.95 * v[i][0] + 0.05 * g * g
        wide = w[i][0].astype(F32)
        step = mm * lax.rsqrt(vv + 1e-8) + 0.1 * wide
        w_out[i][0] = (wide - 0.02 * step).astype(BF16)
        m_out[i][0] = mm
        v_out[i][0] = vv


def adamw(layer, block, factor, grads, weights, m, v, so_far):
    d, width = grads[0].shape
    at = jnp.stack([jnp.int32(layer), jnp.asarray(block, jnp.int32)])
    rows, down_rows = d // STEPS, width // STEPS
    by_column = pl.BlockSpec((rows, width), lambda i, at, f: (i, 0))
    by_row = pl.BlockSpec((down_rows, d), lambda i, at, f: (i, 0))
    column = pl.BlockSpec((1, rows, width), lambda i, at, f: (at[0], i, at[1]))
    row = pl.BlockSpec((1, down_rows, d), lambda i, at, f: (at[0], at[1] * STEPS + i, 0))
    whole = [column, column, row]
    shapes = [jax.ShapeDtypeStruct(a.shape, t) for t in (BF16, F32, F32) for a in weights]
    olds = () if so_far is None else tuple(so_far)
    elements = 3 * d * width
    return pl.pallas_call(
        adamw_kernel,
        grid_spec=pltpu.PrefetchScalarGridSpec(
            num_scalar_prefetch=2,
            grid=(STEPS,),
            in_specs=[by_column, by_column, by_row] + whole * 3 + [pl.BlockSpec(memory_space=pl.ANY)] * len(olds),
            out_specs=whole * 3,
        ),
        out_shape=shapes,
        input_output_aliases={14 + i: i for i in range(len(olds))},
        compiler_params=pltpu.CompilerParams(dimension_semantics=("arbitrary",), vmem_limit_bytes=40 * 2**20),
        cost_estimate=pl.CostEstimate(flops=elements * 900, bytes_accessed=elements * 22, transcendentals=elements),
        name="adamw",
    )(at, factor, *grads, *weights, *m, *v, *olds)


def solution(mesh):
    n = mesh.shape["dp"]
    right = [(i, (i + 1) % n) for i in range(n)]
    left = [(i, (i - 1) % n) for i in range(n)]

    def around(block):
        half = block.shape[0] // 2
        before, after = lax.ppermute(block, "dp", right), lax.ppermute(block, "dp", left)
        top, bottom = lax.ppermute(before[:half], "dp", right), lax.ppermute(after[half:], "dp", left)
        return before, after, jnp.concatenate([top, bottom])

    def gathered(block):
        me = lax.axis_index("dp")
        before, after, far = around(block)
        every = jnp.zeros((n, *block.shape), block.dtype)
        for away, part in ((0, block), (n - 1, before), (1, after), (2, far)):
            every = lax.dynamic_update_slice(every, part[None], ((me + away) % n, 0, 0))
        return every.reshape(n * block.shape[0], block.shape[1])

    def step(x, dy, *arrays):
        weights, m, v = (arrays[i : i + 3] for i in (0, 3, 6))
        w_gate, w_up, w_down = weights
        layers, d, ff = w_gate.shape
        assert n == 4 and layers == 2
        own = ff // (n + 1) // LANES * LANES
        assert own * (n + 1) == ff
        me = lax.axis_index("dp")
        x, dy = x[0], dy[0]

        dy_all = gathered(dy)
        a = normed(x)
        hidden = (jax.nn.silu(dot(a, w_gate[0])) * dot(a, w_up[0])).astype(BF16)
        h = x + dot(hidden, w_down[0]).astype(BF16)
        h_all = gathered(h)
        a, back = jax.vjp(normed, h)
        _, by_gate, by_up = gated(a, dy, w_gate[1], w_up[1], w_down[1])
        by_a = (dot(by_gate, w_gate[1], 1, 1) + dot(by_up, w_up[1], 1, 1)).astype(BF16)
        by_h = dy + back(by_a)[0]
        x_all = gathered(x)
        by_h_all = gathered(by_h)

        def units(w, axis):
            return jnp.concatenate([lax.dynamic_slice_in_dim(w, me * own, own, axis), lax.slice_in_dim(w, n * own, ff, axis=axis)], axis)

        grads = [None] * layers
        squares, common = jnp.float32(0), jnp.float32(0)
        for number, (inputs, outs) in reversed(list(enumerate(((x_all, by_h_all), (h_all, dy_all))))):
            a = normed(inputs)
            hidden, by_gate, by_up = gated(a, outs, units(w_gate[number], 1), units(w_up[number], 1), units(w_down[number], 0))
            down = dot(hidden, outs, 0, 0).astype(BF16)
            gate, up = dot(a, by_gate, 0, 0).astype(BF16), dot(a, by_up, 0, 0).astype(BF16)
            mine = (gate[:, :own], up[:, :own], down[:own])
            shared = (gate[:, own:], up[:, own:], down[own:])
            squares += sum(jnp.sum(g.astype(F32) ** 2) for g in mine)
            common += sum(jnp.sum(g.astype(F32) ** 2) for g in shared)
            others = [around(g) for g in mine]
            grads[number] = [(me, mine), (n, shared)] + [
                ((me + away) % n, tuple(o[i] for o in others)) for i, away in enumerate((n - 1, 1, 2))
            ]
        count = sum(w.size for w in weights)
        total = lax.psum(squares, "dp") + common
        factor = jnp.minimum(1.0, 0.5 * lax.rsqrt(total / count + 1e-30)).reshape(1)

        new = None
        for i in range(n + 1):
            for number in reversed(range(layers)):
                block, g = grads[number][i]
                new = adamw(number, block, factor, g, weights, m, v, new)
        return tuple(new)

    return jax.shard_map(
        step,
        mesh=mesh,
        in_specs=(P(("rep", "dp"), None, None),) * 2 + (P(None, None, None),) * 9,
        out_specs=(P("rep", None, None),) * 9,
        check_vma=False,
    )
```

```python
import functools

import jax
import jax.numpy as jnp
from jax import lax
from jax.experimental import pallas as pl
from jax.experimental.pallas import tpu as pltpu
from jax.sharding import PartitionSpec as P

F32, BF16 = jnp.float32, jnp.bfloat16
ANY, VMEM = pl.ANY, pltpu.VMEM
LANES = 128
WIDE = 512
TILE = 256
ROWS = 512
FEW = 128
TURN = 256
OWN = (640, 384)


def dot(a, b, da=1, db=0):
    return lax.dot_general(a, b, (((da,), (db,)), ((), ())), preferred_element_type=F32)


def aligned(i, size):
    return pl.multiple_of(i * size, size)


def scale_of(wide):
    return lax.rsqrt(jnp.mean(wide**2, -1, keepdims=True) + 1e-6)


def gated(a, dout, w_gate, w_up, w_down):
    gate, up = dot(a, w_gate), dot(a, w_up)
    by_hidden = dot(dout, w_down, 1, 1).astype(BF16).astype(F32)
    s = jax.nn.sigmoid(gate)
    silu = gate * s
    hidden = (silu * up).astype(BF16)
    by_up = (by_hidden * silu).astype(BF16)
    by_gate = (by_hidden * up * (s * (1 + gate * (1 - s)))).astype(BF16)
    return hidden, by_gate, by_up


def gradients_kernel(
    n, count, x, dy, w_gate, w_up, w_down,
    first_gate, first_up, first_down, common_gate, common_up, common_down, last_gate, last_up, last_down, factor,
    x_all, dy_all, h_all, by_all, h_own, by_own,
    a_all, d_all, a_t, d_t, chain_gate, chain_up, chain_down, unit_gate, unit_up, unit_down, out_gate, out_up, out_down,
    hidden, by_gate, by_up, total, squares, square,
    chain_sem, unit_sem, out_sem, load_sem, send_sem, recv_sem, square_send, square_recv,
):
    tokens, d = x.shape
    ff = w_gate.shape[2]
    half = tokens // 2
    me = lax.axis_index("dp")
    right, left, far = lax.rem(me + 1, n), lax.rem(me + n - 1, n), lax.rem(me + 2, n)

    barrier = pltpu.get_barrier_semaphore()
    for other in (right, left, far):
        pl.semaphore_signal(barrier, inc=1, device_id={"dp": other}, device_id_type=pl.DeviceIdType.MESH)
    pl.semaphore_wait(barrier, n - 1)

    def send(src, dst, sems, to):
        return pltpu.make_async_remote_copy(
            src_ref=src, dst_ref=dst, send_sem=sems[0], recv_sem=sems[1], device_id={"dp": to}, device_id_type=pl.DeviceIdType.MESH
        )

    def ring(number, own, place):
        sems = [(send_sem.at[number + k], recv_sem.at[number + k]) for k in range(4)]
        return (
            (send(own, place(me), sems[0], right), send(own, place(me), sems[1], left)),
            (send(place(left, 0), place(left, 0), sems[2], right), send(place(right, 1), place(right, 1), sems[3], left)),
        )

    def block_of(every):
        return lambda i, k=None: every.at[i] if k is None else every.at[i, pl.ds(k * half, half)]

    def columns_of(full, own):
        def place(i, k=None):
            columns = pl.ds(pl.multiple_of(i * own, LANES), own)
            return full.at[:, columns] if k is None else full.at[pl.ds(k * (d // 2), d // 2), columns]

        return place

    def rows_of(full, own):
        def place(i, k=None):
            if k is None:
                return full.at[pl.ds(pl.multiple_of(i * own, LANES), own)]
            return full.at[pl.ds(pl.multiple_of(i * own + k * (own // 2), own // 2), own // 2)]

        return place

    def start(copies):
        for copy in copies:
            copy.start()

    def wait(copies):
        for copy in copies:
            copy.wait()

    def run(copies):
        start(copies)
        wait(copies)

    dy_ring = ring(0, dy, block_of(dy_all))
    x_ring = ring(4, x, block_of(x_all))
    h_ring = ring(8, h_own, block_of(h_all))
    by_ring = ring(12, by_own, block_of(by_all))
    places = columns_of(last_gate, OWN[1]), columns_of(last_up, OWN[1]), rows_of(last_down, OWN[1])
    last_rings = [ring(16 + 4 * i, place(me), place) for i, place in enumerate(places)]
    last_steps = [[copy for one in last_rings for copy in one[k]] for k in range(2)]

    start(dy_ring[0])

    own_x, own_dy, own_h, own_by = (pl.ds(i * tokens, tokens) for i in range(4))

    def chain(layer, body):
        tiles, rest = ff // WIDE, ff % WIDE

        def copies(i, slot, width):
            at = pl.multiple_of(i * WIDE, LANES)
            return [
                pltpu.make_async_copy(w_gate.at[layer, :, pl.ds(at, width)], chain_gate.at[slot, :, pl.ds(0, width)], chain_sem.at[slot, 0]),
                pltpu.make_async_copy(w_up.at[layer, :, pl.ds(at, width)], chain_up.at[slot, :, pl.ds(0, width)], chain_sem.at[slot, 1]),
                pltpu.make_async_copy(w_down.at[layer, pl.ds(at, width)], chain_down.at[slot, pl.ds(0, width)], chain_sem.at[slot, 2]),
            ]

        def rows_loop(slot, width):
            def some(r, _):
                body(pl.ds(pl.multiple_of(r * ROWS, ROWS), ROWS), slot, width)
                return 0

            lax.fori_loop(0, tokens // ROWS, some, 0)

        def tile(i, _):
            slot = lax.rem(i, 2)
            wait(copies(i, slot, WIDE))

            @pl.when(i + 1 < tiles)
            def _():
                start(copies(i + 1, lax.rem(i + 1, 2), WIDE))

            if rest:

                @pl.when(i + 1 == tiles)
                def _():
                    start(copies(tiles, tiles % 2, rest))

            rows_loop(slot, WIDE)
            return 0

        start(copies(0, 0, WIDE))
        total[...] = jnp.zeros_like(total)
        lax.fori_loop(0, tiles, tile, 0)
        if rest:
            wait(copies(tiles, tiles % 2, rest))
            rows_loop(tiles % 2, rest)

    def forward(rows, slot, width):
        a, units = a_all[rows], pl.ds(0, width)
        gate, up = dot(a, chain_gate[slot, :, units]), dot(a, chain_up[slot, :, units])
        total[rows] += dot((jax.nn.silu(gate) * up).astype(BF16), chain_down[slot, units])

    def backward(rows, slot, width):
        units = pl.ds(0, width)
        to_gate, to_up = chain_gate[slot, :, units], chain_up[slot, :, units]
        there = pl.ds(pl.multiple_of(tokens + rows.start, ROWS), ROWS)
        _, gate, up = gated(a_all[rows], d_all[there], to_gate, to_up, chain_down[slot, units])
        total[rows] += dot(gate, to_gate, 1, 1) + dot(up, to_up, 1, 1)

    def each(rows, body, length=tokens):
        def some(r, _):
            body(pl.multiple_of(r * rows, rows))
            return 0

        lax.fori_loop(0, length // rows, some, 0)

    def at(part, r, rows):
        return pl.ds(pl.multiple_of(part * tokens + r, rows), rows)

    run(
        [
            pltpu.make_async_copy(x, d_all.at[own_x], load_sem.at[0]),
            pltpu.make_async_copy(dy, d_all.at[own_dy], load_sem.at[1]),
        ]
    )

    def norm_x(r):
        wide = d_all[at(0, r, FEW)].astype(F32)
        a_all[at(0, r, FEW)] = (wide * scale_of(wide)).astype(BF16)

    each(FEW, norm_x)
    chain(0, forward)

    def add_layer(r):
        h = d_all[at(0, r, FEW)] + total[at(0, r, FEW)].astype(BF16)
        d_all[at(2, r, FEW)] = h
        wide = h.astype(F32)
        a_all[at(0, r, FEW)] = (wide * scale_of(wide)).astype(BF16)

    each(FEW, add_layer)
    run([pltpu.make_async_copy(d_all.at[own_h], h_own, load_sem.at[0])])
    start(h_ring[0])
    chain(1, backward)

    def norm_back(r):
        wide = d_all[at(2, r, FEW)].astype(F32)
        scale = scale_of(wide)
        by_a = total[at(0, r, FEW)].astype(BF16).astype(F32)
        by_mean = jnp.sum(by_a * wide, -1, keepdims=True) * -0.5 * (scale * scale * scale)
        by_wide = by_a * scale + wide * (by_mean * (2.0 / d))
        d_all[at(3, r, FEW)] = d_all[at(1, r, FEW)] + by_wide.astype(BF16)

    each(FEW, norm_back)
    run([pltpu.make_async_copy(d_all.at[own_by], by_own, load_sem.at[0])])

    def load(states, own_states, outs, own_outs):
        copies = []
        for which, (every, own, there) in enumerate(((states, own_states, a_all), (outs, own_outs, d_all))):
            for away in range(n):
                i = lax.rem(me + away, n)
                rows = there.at[pl.ds(pl.multiple_of(i * tokens, tokens), tokens)]
                copies.append(pltpu.make_async_copy(own if away == 0 else every.at[i], rows, load_sem.at[which * n + away]))
        run(copies)

        def turn(r):
            rows = pl.ds(r, TURN)
            wide = a_all[rows].astype(F32)
            a = (wide * scale_of(wide)).astype(BF16)
            a_all[rows] = a
            a_t[:, rows] = a.T
            d_t[:, rows] = d_all[rows].T

        each(TURN, turn, n * tokens)

    squares[...] = jnp.zeros_like(squares)

    def gradients(layer, targets, between):
        mine = OWN[layer] // LANES
        lots = ff // LANES - (n - 1) * mine
        per = TILE // LANES
        tiles = lots // per

        def units(g):
            return pl.ds(pl.multiple_of(jnp.where(g < mine, me * mine + g, (n - 1) * mine + g) * LANES, LANES), LANES)

        def weight_copies(i, slot):
            copies = []
            for p in range(per):
                there, part = units(i * per + p), pl.ds(p * LANES, LANES)
                copies += [
                    pltpu.make_async_copy(w_gate.at[layer, :, there], unit_gate.at[slot, :, part], unit_sem.at[slot, 3 * p]),
                    pltpu.make_async_copy(w_up.at[layer, :, there], unit_up.at[slot, :, part], unit_sem.at[slot, 3 * p + 1]),
                    pltpu.make_async_copy(w_down.at[layer, there], unit_down.at[slot, part], unit_sem.at[slot, 3 * p + 2]),
                ]
            return copies

        def put(i, slot, act):
            for p in range(per):
                part = pl.ds(p * LANES, LANES)
                for condition, (to_gate, to_up, to_down) in targets(i * per + p, units(i * per + p)):
                    copies = [
                        pltpu.make_async_copy(out_gate.at[slot, :, part], to_gate, out_sem.at[slot, 3 * p]),
                        pltpu.make_async_copy(out_up.at[slot, :, part], to_up, out_sem.at[slot, 3 * p + 1]),
                        pltpu.make_async_copy(out_down.at[slot, part], to_down, out_sem.at[slot, 3 * p + 2]),
                    ]
                    if condition is None:
                        act(copies)
                    else:
                        pl.when(condition)(functools.partial(act, copies))

        def tile(i, _):
            slot = lax.rem(i, 2)
            wait(weight_copies(i, slot))

            @pl.when(i + 1 < tiles)
            def _():
                start(weight_copies(i + 1, lax.rem(i + 1, 2)))

            between(i)

            def some(r, _):
                rows = pl.ds(pl.multiple_of(r * ROWS, ROWS), ROWS)
                made = gated(a_all[rows], d_all[rows], unit_gate[slot], unit_up[slot], unit_down[slot])
                hidden[rows], by_gate[rows], by_up[rows] = made
                return 0

            lax.fori_loop(0, n * tokens // ROWS, some, 0)

            @pl.when(i >= 2)
            def _():
                put(i - 2, slot, wait)

            both = jnp.zeros((8, TILE), F32)
            for turned, by, out in ((a_t, by_gate, out_gate), (a_t, by_up, out_up), (d_t, hidden, out_down)):
                g = dot(turned[...], by[...]).astype(BF16)
                out[slot] = g.T if out is out_down else g
                wide = g.astype(F32)
                both += jnp.sum((wide * wide).reshape(d // 8, 8, TILE), 0)
            for p in range(per):
                part, is_mine = both[:, p * LANES : (p + 1) * LANES], i * per + p < mine
                squares[0] += jnp.where(is_mine, part, 0.0)
                squares[1] += jnp.where(is_mine, 0.0, part)
            put(i, slot, start)
            return 0

        start(weight_copies(0, 0))
        lax.fori_loop(0, tiles, tile, 0)
        for i in range(max(tiles - 2, 0), tiles):
            put(i, i % 2, wait)

    wait(dy_ring[0])
    start(dy_ring[1])
    wait(h_ring[0])
    start(h_ring[1])
    start(by_ring[0])
    start(x_ring[0])
    wait(dy_ring[1])
    wait(h_ring[1])
    load(h_all, h_own, dy_all, dy)

    def forward_on(i):
        @pl.when(i == 3)
        def _():
            wait(by_ring[0])
            start(by_ring[1])

        @pl.when(i == 6)
        def _():
            wait(x_ring[0])
            start(x_ring[1])

    gradients(1, lambda g, units: [(None, (last_gate.at[:, units], last_up.at[:, units], last_down.at[units]))], forward_on)
    start(last_steps[0])
    wait(by_ring[1])
    wait(x_ring[1])
    load(x_all, x, by_all, by_own)

    def first_targets(g, units):
        mine = OWN[0] // LANES
        own = pl.ds(pl.multiple_of(jnp.minimum(g, mine - 1) * LANES, LANES), LANES)
        rest = pl.ds(pl.multiple_of(jnp.maximum(g - mine, 0) * LANES, LANES), LANES)
        return [
            (g < mine, (first_gate.at[:, own], first_up.at[:, own], first_down.at[own])),
            (g >= mine, (common_gate.at[:, rest], common_up.at[:, rest], common_down.at[rest])),
        ]

    def last_on(i):
        @pl.when(i == 3)
        def _():
            wait(last_steps[0])
            start(last_steps[1])

    gradients(0, first_targets, last_on)

    square[me] = squares[0]
    swaps = [send(square.at[me], square.at[me], (square_send.at[k], square_recv.at[k]), to) for k, to in enumerate((right, left, far))]
    start(swaps)
    wait(swaps)
    wait(last_steps[1])
    every = squares[1]
    for i in range(n):
        every = every + square[i]
    every = jnp.sum(jnp.sum(every, 0, keepdims=True), 1, keepdims=True)
    factor[...] = jnp.broadcast_to(jnp.minimum(1.0, 0.5 * lax.rsqrt(every / count + 1e-30)), factor.shape)


def make_gradients(n, x, dy, w_gate, w_up, w_down):
    tokens, d = x.shape
    layers, _, ff = w_gate.shape
    assert n == 4 and layers == 2
    own, rest = OWN[0], ff - n * OWN[0]
    shape = jax.ShapeDtypeStruct
    every = shape((n, tokens, d), BF16)
    outs = [shape((d, own), BF16)] * 2 + [shape((own, d), BF16)] + [shape((d, rest), BF16)] * 2 + [shape((rest, d), BF16)]
    outs += [shape((d, ff), BF16)] * 2 + [shape((ff, d), BF16)] + [shape((8, LANES), F32)] + [every] * 4 + [shape((tokens, d), BF16)] * 2
    dma = pltpu.SemaphoreType.DMA
    scratch = [VMEM((n * tokens, d), BF16)] * 2 + [VMEM((d, n * tokens), BF16)] * 2
    scratch += [VMEM((2, d, WIDE), BF16)] * 2 + [VMEM((2, WIDE, d), BF16)]
    scratch += ([VMEM((2, d, TILE), BF16)] * 2 + [VMEM((2, TILE, d), BF16)]) * 2
    scratch += [VMEM((n * tokens, TILE), BF16)] * 3 + [VMEM((tokens, d), F32), VMEM((2, 8, LANES), F32), VMEM((n, 8, LANES), F32)]
    scratch += [dma((2, 3)), dma((2, 6)), dma((2, 6)), dma((2 * n,)), dma((28,)), dma((28,)), dma((3,)), dma((3,))]
    return pl.pallas_call(
        functools.partial(gradients_kernel, n, layers * 3 * d * ff),
        out_shape=outs,
        in_specs=[pl.BlockSpec(memory_space=ANY)] * 5,
        out_specs=[pl.BlockSpec(memory_space=ANY)] * 9 + [pl.BlockSpec(memory_space=VMEM)] + [pl.BlockSpec(memory_space=ANY)] * 6,
        scratch_shapes=scratch,
        compiler_params=pltpu.CompilerParams(collective_id=0, has_side_effects=True, vmem_limit_bytes=67043328),
        cost_estimate=pl.CostEstimate(flops=tokens * d * ff * 2 * 40, bytes_accessed=2**27, transcendentals=0),
        name="gradients",
    )(x, dy, w_gate, w_up, w_down)[:10]


def adamw_kernel(*refs):
    factor, grads, w, m, v = (refs[1], *(refs[i : i + 3] for i in (2, 5, 8, 11)))
    w_out, m_out, v_out = (refs[len(refs) - 9 + i : len(refs) - 6 + i] for i in (0, 3, 6))
    c = factor[0:1, 0:1]
    for i in range(3):
        g = grads[i][...].astype(F32) * c
        mm = 0.9 * m[i][0] + 0.1 * g
        vv = 0.95 * v[i][0] + 0.05 * g * g
        wide = w[i][0].astype(F32)
        step = mm * lax.rsqrt(vv + 1e-8) + 0.1 * wide
        w_out[i][0] = (wide - 0.02 * step).astype(BF16)
        m_out[i][0] = mm
        v_out[i][0] = vv


def adamw(layer, block, steps, factor, grads, weights, m, v, so_far):
    d, width = grads[0].shape
    at = jnp.asarray(block, jnp.int32).reshape(1)
    rows, down_rows = d // steps, width // steps
    by_column = pl.BlockSpec((rows, width), lambda i, at: (i, 0))
    by_row = pl.BlockSpec((down_rows, d), lambda i, at: (i, 0))
    column = pl.BlockSpec((1, rows, width), lambda i, at: (layer, i, at[0]))
    row = pl.BlockSpec((1, down_rows, d), lambda i, at: (layer, at[0] * steps + i, 0))
    whole = [column, column, row]
    shapes = [jax.ShapeDtypeStruct(a.shape, t) for t in (BF16, F32, F32) for a in weights]
    olds = () if so_far is None else tuple(so_far)
    elements = 3 * d * width
    return pl.pallas_call(
        adamw_kernel,
        grid_spec=pltpu.PrefetchScalarGridSpec(
            num_scalar_prefetch=1,
            grid=(steps,),
            in_specs=[pl.BlockSpec((8, LANES), lambda i, at: (0, 0)), by_column, by_column, by_row]
            + whole * 3
            + [pl.BlockSpec(memory_space=ANY)] * len(olds),
            out_specs=whole * 3,
        ),
        out_shape=shapes,
        input_output_aliases={14 + i: i for i in range(len(olds))},
        compiler_params=pltpu.CompilerParams(dimension_semantics=("arbitrary",), vmem_limit_bytes=56 * 2**20),
        cost_estimate=pl.CostEstimate(flops=elements * 900, bytes_accessed=elements * 22, transcendentals=elements),
        name="adamw",
    )(at, factor, *grads, *weights, *m, *v, *olds)


def solution(mesh):
    n = mesh.shape["dp"]
    to_right = [(i, (i + 1) % n) for i in range(n)]
    to_left = [(i, (i - 1) % n) for i in range(n)]

    def step(x, dy, *arrays):
        weights, m, v = (arrays[i : i + 3] for i in (0, 3, 6))
        me = lax.axis_index("dp")
        *gradients, factor = make_gradients(n, x[0], dy[0], *weights)
        mine, common, last = (gradients[i : i + 3] for i in (0, 3, 6))
        before = [lax.ppermute(g, "dp", to_right) for g in mine]
        after = [lax.ppermute(g, "dp", to_left) for g in mine]

        def update(layer, block, steps, g, new):
            return adamw(layer, block, steps, factor, g, weights, m, v, new)

        new = update(1, 0, 16, last, None)
        new = update(0, me, 8, mine, new)
        new = update(0, n, 8, common, new)
        top = [lax.ppermute(g[: g.shape[0] // 2], "dp", to_right) for g in before]
        bottom = [lax.ppermute(g[g.shape[0] // 2 :], "dp", to_left) for g in after]
        new = update(0, (me + n - 1) % n, 8, before, new)
        new = update(0, (me + 1) % n, 8, after, new)
        far = [jnp.concatenate(both) for both in zip(top, bottom, strict=True)]
        new = update(0, (me + 2) % n, 8, far, new)
        return tuple(new)

    return jax.shard_map(
        step,
        mesh=mesh,
        in_specs=(P(("rep", "dp"), None, None),) * 2 + (P(None, None, None),) * 9,
        out_specs=(P("rep", None, None),) * 9,
        check_vma=False,
    )
```

```python
import functools

import jax
import jax.numpy as jnp
from jax import lax
from jax.experimental import pallas as pl
from jax.experimental.pallas import tpu as pltpu
from jax.sharding import PartitionSpec as P

F32, BF16 = jnp.float32, jnp.bfloat16
ANY, VMEM = pl.ANY, pltpu.VMEM
LANES = 128
WIDE = 512
TILE = 256
ROWS = 512
CHAIN_ROWS = 512
FEW = 128
TURN = 256
PIECE_STEPS = 2
FORWARD_AT = 4
OWN = (640, 640)


def dot(a, b, da=1, db=0):
    return lax.dot_general(a, b, (((da,), (db,)), ((), ())), preferred_element_type=F32)


def aligned(i, size):
    return pl.multiple_of(i * size, size)


def scale_of(wide):
    return lax.rsqrt(jnp.mean(wide**2, -1, keepdims=True) + 1e-6)


def gated(a, dout, w_gate, w_up, w_down):
    gate, up = dot(a, w_gate), dot(a, w_up)
    by_hidden = dot(dout, w_down, 1, 1).astype(BF16).astype(F32)
    s = jax.nn.sigmoid(gate)
    silu = gate * s
    hidden = (silu * up).astype(BF16)
    by_up = (by_hidden * silu).astype(BF16)
    by_gate = (by_hidden * up * (s * (1 + gate * (1 - s)))).astype(BF16)
    return hidden, by_gate, by_up


def gradients_kernel(
    n, count, x, dy, w_gate, w_up, w_down,
    first_top, first_bottom, common_top, common_bottom, last_gate, last_up, last_down, factor, x_all, dy_all, by_all, by_own,
    a_all, d_all, a_t, d_t, chain_gate, chain_up, chain_down, unit_gate, unit_up, unit_down, out_gate, out_up, out_down, out_turned,
    hidden, by_gate, by_up, total, squares, square,
    chain_sem, unit_sem, out_sem, first_sem, load_sem, send_sem, recv_sem, square_send, square_recv,
):
    tokens, d = x.shape
    ff = w_gate.shape[2]
    half = tokens // 2
    me = lax.axis_index("dp")
    right, left, far = lax.rem(me + 1, n), lax.rem(me + n - 1, n), lax.rem(me + 2, n)

    barrier = pltpu.get_barrier_semaphore()
    for other in (right, left, far):
        pl.semaphore_signal(barrier, inc=1, device_id={"dp": other}, device_id_type=pl.DeviceIdType.MESH)
    pl.semaphore_wait(barrier, n - 1)

    def send(src, dst, sems, to):
        return pltpu.make_async_remote_copy(
            src_ref=src, dst_ref=dst, send_sem=sems[0], recv_sem=sems[1], device_id={"dp": to}, device_id_type=pl.DeviceIdType.MESH
        )

    def ring(number, own, place):
        sems = [(send_sem.at[number + k], recv_sem.at[number + k]) for k in range(4)]
        return (
            (send(own, place(me), sems[0], right), send(own, place(me), sems[1], left)),
            (send(place(left, 0), place(left, 0), sems[2], right), send(place(right, 1), place(right, 1), sems[3], left)),
        )

    def block_of(every):
        return lambda i, k=None: every.at[i] if k is None else every.at[i, pl.ds(k * half, half)]

    def columns_of(full, own):
        def place(i, k=None):
            columns = pl.ds(pl.multiple_of(i * own, LANES), own)
            return full.at[:, columns] if k is None else full.at[pl.ds(k * (d // 2), d // 2), columns]

        return place

    def rows_of(full, own):
        def place(i, k=None):
            if k is None:
                return full.at[pl.ds(pl.multiple_of(i * own, LANES), own)]
            return full.at[pl.ds(pl.multiple_of(i * own + k * (own // 2), own // 2), own // 2)]

        return place

    def start(copies):
        for copy in copies:
            copy.start()

    def wait(copies):
        for copy in copies:
            copy.wait()

    def run(copies):
        start(copies)
        wait(copies)

    dy_ring = ring(0, dy, block_of(dy_all))
    x_ring = ring(4, x, block_of(x_all))
    by_ring = ring(8, by_own, block_of(by_all))
    places = columns_of(last_gate, OWN[1]), columns_of(last_up, OWN[1]), rows_of(last_down, OWN[1])
    last_rings = [ring(12 + 4 * i, place(me), place) for i, place in enumerate(places)]
    last_steps = [[copy for one in last_rings for copy in one[k]] for k in range(2)]

    start(x_ring[0])
    start(dy_ring[0])

    tiles, rest = ff // WIDE, ff % WIDE

    def chain_copies(layer, i, slot, width):
        there, part = pl.ds(pl.multiple_of(i * WIDE, LANES), width), pl.ds(0, width)
        return [
            pltpu.make_async_copy(w_gate.at[layer, :, there], chain_gate.at[slot, :, part], chain_sem.at[slot, 0]),
            pltpu.make_async_copy(w_up.at[layer, :, there], chain_up.at[slot, :, part], chain_sem.at[slot, 1]),
            pltpu.make_async_copy(w_down.at[layer, there], chain_down.at[slot, part], chain_sem.at[slot, 2]),
        ]

    def chain(layer, body):
        def rows_loop(slot, width):
            def some(r, _):
                body(pl.multiple_of(r * CHAIN_ROWS, CHAIN_ROWS), slot, width)
                return 0

            lax.fori_loop(0, tokens // CHAIN_ROWS, some, 0)

        def tile(i, _):
            slot = lax.rem(i, 2)
            wait(chain_copies(layer, i, slot, WIDE))

            @pl.when(i + 1 < tiles)
            def _():
                start(chain_copies(layer, i + 1, lax.rem(i + 1, 2), WIDE))

            if rest:

                @pl.when(i + 1 == tiles)
                def _():
                    start(chain_copies(layer, tiles, tiles % 2, rest))

            rows_loop(slot, WIDE)
            return 0

        total[...] = jnp.zeros_like(total)
        lax.fori_loop(0, tiles, tile, 0)
        if rest:
            wait(chain_copies(layer, tiles, tiles % 2, rest))
            rows_loop(tiles % 2, rest)

    def forward(r, slot, width):
        rows, units = pl.ds(r, CHAIN_ROWS), pl.ds(0, width)
        a = d_all[at(1, r, CHAIN_ROWS)]
        gate, up = dot(a, chain_gate[slot, :, units]), dot(a, chain_up[slot, :, units])
        total[rows] += dot((jax.nn.silu(gate) * up).astype(BF16), chain_down[slot, units])

    def backward(r, slot, width):
        rows, units = pl.ds(r, CHAIN_ROWS), pl.ds(0, width)
        to_gate, to_up = chain_gate[slot, :, units], chain_up[slot, :, units]
        a, by = a_all[at(me, r, CHAIN_ROWS)], d_all[at(2, r, CHAIN_ROWS)]
        _, gate, up = gated(a, by, to_gate, to_up, chain_down[slot, units])
        total[rows] += dot(gate, to_gate, 1, 1) + dot(up, to_up, 1, 1)

    def each(rows, body, length=tokens):
        def some(r, _):
            body(pl.multiple_of(r * rows, rows))
            return 0

        lax.fori_loop(0, length // rows, some, 0)

    def at(part, r, rows):
        return pl.ds(pl.multiple_of(part * tokens + r, rows), rows)

    def part(i):
        return d_all.at[pl.ds(i * tokens, tokens)]

    def norm_back(r):
        wide = d_all[at(3, r, FEW)].astype(F32)
        scale = scale_of(wide)
        by_a = total[at(0, r, FEW)].astype(BF16).astype(F32)
        by_mean = jnp.sum(by_a * wide, -1, keepdims=True) * -0.5 * (scale * scale * scale)
        by_wide = by_a * scale + wide * (by_mean * (2.0 / d))
        d_all[at(3, r, FEW)] = d_all[at(2, r, FEW)] + by_wide.astype(BF16)

    def take(src, to, sem):
        return [pltpu.make_async_copy(src, part(to), load_sem.at[sem])]

    def sequence(i, _):
        whose = jnp.where(i == 0, me, jnp.where(i == 1, left, jnp.where(i == 2, right, far)))
        states = jnp.where(i == 2, 2, 0)

        @pl.when(i == 0)
        def _():
            wait(take(x, 0, 0))

        @pl.when(i == 1)
        def _():
            wait(take(x_all.at[left], 0, 0))

        @pl.when(i == 2)
        def _():
            wait(take(x_all.at[right], 2, 1))

        @pl.when(i == 3)
        def _():
            wait(take(x_all.at[far], 0, 0))

        def norm_x(r):
            wide = d_all[at(states, r, FEW)].astype(F32)
            d_all[at(1, r, FEW)] = (wide * scale_of(wide)).astype(BF16)

        each(FEW, norm_x)
        chain(0, forward)

        @pl.when(i == 0)
        def _():
            start(chain_copies(1, 0, 0, WIDE))

        @pl.when((i == 1) | (i == 2))
        def _():
            start(chain_copies(0, 0, 0, WIDE))

        @pl.when(i == 2)
        def _():
            wait(x_ring[1])
            start(take(x_all.at[far], 0, 0))

        @pl.when(i == 1)
        def _():
            wait(dy_ring[0])
            start(dy_ring[1])
            start(by_ring[0])

        def add_layer(r):
            h = d_all[at(states, r, FEW)] + total[at(0, r, FEW)].astype(BF16)
            d_all[at(3, r, FEW)] = h
            wide = h.astype(F32)
            a_all[at(whose, r, FEW)] = (wide * scale_of(wide)).astype(BF16)

        each(FEW, add_layer)

        @pl.when(i == 0)
        def _():
            wait(take(dy, 2, 1))
            chain(1, backward)
            start(chain_copies(0, 0, 0, WIDE))
            wait(x_ring[0])
            start(x_ring[1])
            start(take(x_all.at[left], 0, 0))
            each(FEW, norm_back)
            start(take(x_all.at[right], 2, 1))
            run([pltpu.make_async_copy(part(3), by_own, load_sem.at[2])])

        return 0

    start(take(x, 0, 0) + take(dy, 2, 1) + chain_copies(0, 0, 0, WIDE))
    lax.fori_loop(0, n, sequence, 0)

    def load(every, own, there, sem):
        copies = []
        for away in range(n):
            i = lax.rem(me + away, n)
            rows = there.at[pl.ds(pl.multiple_of(i * tokens, tokens), tokens)]
            copies.append(pltpu.make_async_copy(own if away == 0 else every.at[i], rows, load_sem.at[sem + away]))
        return copies

    def turn_states(r):
        a_t[:, pl.ds(r, TURN)] = a_all[pl.ds(r, TURN)].T

    def norm_states(r):
        rows = pl.ds(r, TURN)
        wide = a_all[rows].astype(F32)
        a = (wide * scale_of(wide)).astype(BF16)
        a_all[rows] = a
        a_t[:, rows] = a.T

    def turn_outs(r):
        d_t[:, pl.ds(r, TURN)] = d_all[pl.ds(r, TURN)].T

    squares[...] = jnp.zeros_like(squares)

    def plan(layer):
        mine = OWN[layer] // LANES
        lots = ff // LANES - (n - 1) * mine
        per = TILE // LANES
        count = pl.cdiv(lots, per)

        def units(g):
            g = jnp.minimum(g, lots - 1)
            return pl.ds(pl.multiple_of(jnp.where(g < mine, me * mine + g, (n - 1) * mine + g) * LANES, LANES), LANES)

        def weight_copies(i, slot):
            copies = []
            for p in range(per):
                there, part = units(i * per + p), pl.ds(p * LANES, LANES)
                copies += [
                    pltpu.make_async_copy(w_gate.at[layer, :, there], unit_gate.at[slot, :, part], unit_sem.at[slot, 3 * p]),
                    pltpu.make_async_copy(w_up.at[layer, :, there], unit_up.at[slot, :, part], unit_sem.at[slot, 3 * p + 1]),
                    pltpu.make_async_copy(w_down.at[layer, there], unit_down.at[slot, part], unit_sem.at[slot, 3 * p + 2]),
                ]
            return copies

        return mine, lots, per, count, units, weight_copies

    def first_weights(layer):
        return plan(layer)[-1](0, 0)

    def gradients(layer, targets, between, after):
        mine, lots, per, tiles, units, weight_copies = plan(layer)

        def put(i, slot, act):
            for p in range(per):
                for condition, copies in targets(i * per + p, units(i * per + p), slot, pl.ds(p * LANES, LANES), 4 * p):
                    pl.when(condition & (i * per + p < lots))(functools.partial(act, copies))

        def tile(i, _):
            slot = lax.rem(i, 2)
            wait(weight_copies(i, slot))

            @pl.when(i + 1 < tiles)
            def _():
                start(weight_copies(i + 1, lax.rem(i + 1, 2)))

            @pl.when(i >= 2)
            def _():
                put(i - 2, slot, wait)

            between(i)

            def some(r, _):
                rows = pl.ds(pl.multiple_of(r * ROWS, ROWS), ROWS)
                made = gated(a_all[rows], d_all[rows], unit_gate[slot], unit_up[slot], unit_down[slot])
                hidden[rows], by_gate[rows], by_up[rows] = made
                return 0

            lax.fori_loop(0, n * tokens // ROWS, some, 0)
            pl.when(i == tiles - 1)(after)

            both = jnp.zeros((8, TILE), F32)
            for turned, by, out in ((a_t, by_gate, out_gate), (a_t, by_up, out_up), (d_t, hidden, out_down)):
                g = dot(turned[...], by[...]).astype(BF16)
                if out is out_down and layer:
                    out[slot] = g.T
                elif out is out_down:
                    out_turned[slot] = g
                else:
                    out[slot] = g
                wide = g.astype(F32)
                both += jnp.sum((wide * wide).reshape(d // 8, 8, TILE), 0)
            for p in range(per):
                part, g = both[:, p * LANES : (p + 1) * LANES], i * per + p
                squares[0] += jnp.where(g < mine, part, 0.0)
                squares[1] += jnp.where((g >= mine) & (g < lots), part, 0.0)
            put(i, slot, start)
            return 0

        lax.fori_loop(0, tiles, tile, 0)
        for i in range(max(tiles - 2, 0), tiles):
            put(i, i % 2, wait)

    wait(dy_ring[1])
    start(load(dy_all, dy, d_all, n))
    start(first_weights(1))
    each(TURN, turn_states, n * tokens)
    wait(load(dy_all, dy, d_all, n))
    each(TURN, turn_outs, n * tokens)

    def last_targets(g, units, slot, part, sem):
        return [
            (
                g >= 0,
                [
                    pltpu.make_async_copy(out_gate.at[slot, :, part], last_gate.at[:, units], out_sem.at[slot, sem]),
                    pltpu.make_async_copy(out_up.at[slot, :, part], last_up.at[:, units], out_sem.at[slot, sem + 1]),
                    pltpu.make_async_copy(out_down.at[slot, part], last_down.at[units], out_sem.at[slot, sem + 2]),
                ],
            )
        ]

    def forward_on(i):
        @pl.when(i == 1)
        def _():
            wait(by_ring[0])
            start(by_ring[1])

        @pl.when(i == pl.cdiv(OWN[1], TILE) + 1)
        def _():
            start(last_steps[0])

    def load_first():
        wait(by_ring[1])
        start(load(x_all, x, a_all, 0) + load(by_all, by_own, d_all, n))

    gradients(1, last_targets, forward_on, load_first)
    start(first_weights(0))
    wait(load(x_all, x, a_all, 0) + load(by_all, by_own, d_all, n))
    each(TURN, norm_states, n * tokens)
    each(TURN, turn_outs, n * tokens)

    def first_targets(g, units, slot, part, sem):
        mine = OWN[0] // LANES

        def copies(top, bottom, at):
            columns = pl.ds(pl.multiple_of(at * LANES, LANES), LANES)
            made = []
            for k, to in enumerate((top, bottom)):
                for which, out in enumerate((out_gate, out_up, out_turned)):
                    some = out.at[slot, pl.ds(k * (d // 2), d // 2), part]
                    made.append(pltpu.make_async_copy(some, to.at[which, :, columns], first_sem.at[slot, sem // 4 * 6 + 3 * k + which]))
            return made

        return [
            (g < mine, copies(first_top, first_bottom, jnp.minimum(g, mine - 1))),
            (g >= mine, copies(common_top, common_bottom, jnp.maximum(g - mine, 0))),
        ]

    def last_on(i):
        @pl.when(i == FORWARD_AT)
        def _():
            wait(last_steps[0])
            start(last_steps[1])

    gradients(0, first_targets, last_on, lambda: None)

    square[me] = squares[0]
    swaps = [send(square.at[me], square.at[me], (square_send.at[k], square_recv.at[k]), to) for k, to in enumerate((right, left, far))]
    start(swaps)
    wait(swaps)
    wait(last_steps[1])
    every = squares[1]
    for i in range(n):
        every = every + square[i]
    every = jnp.sum(jnp.sum(every, 0, keepdims=True), 1, keepdims=True)
    factor[...] = jnp.broadcast_to(jnp.minimum(1.0, 0.5 * lax.rsqrt(every / count + 1e-30)), factor.shape)


def make_gradients(n, x, dy, w_gate, w_up, w_down):
    tokens, d = x.shape
    layers, _, ff = w_gate.shape
    assert n == 4 and layers == 2
    own, rest = OWN[0], ff - n * OWN[0]
    shape = jax.ShapeDtypeStruct
    every = shape((n, tokens, d), BF16)
    outs = [shape((3, d // 2, own), BF16)] * 2 + [shape((3, d // 2, rest), BF16)] * 2
    outs += [shape((d, ff), BF16)] * 2 + [shape((ff, d), BF16)] + [shape((8, LANES), F32)] + [every] * 3 + [shape((tokens, d), BF16)]
    dma = pltpu.SemaphoreType.DMA
    scratch = [VMEM((n * tokens, d), BF16)] * 2 + [VMEM((d, n * tokens), BF16)] * 2
    scratch += [VMEM((2, d, WIDE), BF16)] * 2 + [VMEM((2, WIDE, d), BF16)]
    scratch += ([VMEM((2, d, TILE), BF16)] * 2 + [VMEM((2, TILE, d), BF16)]) * 2 + [VMEM((2, d, TILE), BF16)]
    scratch += [VMEM((n * tokens, TILE), BF16)] * 3 + [VMEM((tokens, d), F32), VMEM((2, 8, LANES), F32), VMEM((n, 8, LANES), F32)]
    scratch += [dma((2, 3)), dma((2, 6)), dma((2, 8)), dma((2, 12)), dma((2 * n,)), dma((24,)), dma((24,)), dma((3,)), dma((3,))]
    return pl.pallas_call(
        functools.partial(gradients_kernel, n, layers * 3 * d * ff),
        out_shape=outs,
        in_specs=[pl.BlockSpec(memory_space=ANY)] * 5,
        out_specs=[pl.BlockSpec(memory_space=ANY)] * 7 + [pl.BlockSpec(memory_space=VMEM)] + [pl.BlockSpec(memory_space=ANY)] * 4,
        scratch_shapes=scratch,
        compiler_params=pltpu.CompilerParams(collective_id=0, has_side_effects=True, vmem_limit_bytes=67043328),
        cost_estimate=pl.CostEstimate(flops=tokens * d * ff * 2 * 40, bytes_accessed=2**27, transcendentals=0),
        name="gradients",
    )(x, dy, w_gate, w_up, w_down)[:8]


def adamw_update(g, w, m, v, w_out, m_out, v_out):
    m = 0.9 * m[0] + 0.1 * g
    v = 0.95 * v[0] + 0.05 * g * g
    wide = w[0].astype(F32)
    step = m * lax.rsqrt(v + 1e-8) + 0.1 * wide
    w_out[0] = (wide - 0.02 * step).astype(BF16)
    m_out[0] = m
    v_out[0] = v


def whole_kernel(factor, *refs):
    grads, w, m, v = (refs[i : i + 3] for i in (0, 3, 6, 9))
    outs = refs[len(refs) - 9 :]
    for i in range(3):
        adamw_update(grads[i][...].astype(F32) * factor[0:1, 0:1], w[i], m[i], v[i], *outs[i::3])


def pieces_kernel(pieces, at, factor, *refs):
    del at
    w, m, v = (refs[i : i + 3] for i in (pieces, pieces + 3, pieces + 6))
    outs = refs[len(refs) - 9 :]
    piece = pl.program_id(0) // PIECE_STEPS
    g = refs[0][...]
    for k in range(1, pieces):
        g = jnp.where(piece >= k, refs[k][...], g)
    for i in range(3):
        own = g[i].T if i == 2 else g[i]
        adamw_update(own.astype(F32) * factor[0:1, 0:1], w[i], m[i], v[i], *outs[i::3])


def adamw_call(kernel, grid, scalars, grads, grad_specs, specs, factor, weights, m, v, so_far):
    shapes = [jax.ShapeDtypeStruct(a.shape, t) for t in (BF16, F32, F32) for a in weights]
    olds = () if so_far is None else tuple(so_far)
    elements = sum(g.size for g in grads)
    first_old = len(scalars) + 1 + len(grads) + 9
    return pl.pallas_call(
        kernel,
        grid_spec=pltpu.PrefetchScalarGridSpec(
            num_scalar_prefetch=len(scalars),
            grid=grid,
            in_specs=[pl.BlockSpec((8, LANES), lambda *_: (0, 0)), *grad_specs, *(specs * 3)] + [pl.BlockSpec(memory_space=ANY)] * len(olds),
            out_specs=specs * 3,
        ),
        out_shape=shapes,
        input_output_aliases={first_old + i: i for i in range(len(olds))},
        compiler_params=pltpu.CompilerParams(dimension_semantics=("arbitrary",), vmem_limit_bytes=56 * 2**20),
        cost_estimate=pl.CostEstimate(flops=elements * 900, bytes_accessed=elements * 22, transcendentals=elements),
        name="adamw",
    )(*scalars, factor, *grads, *weights, *m, *v, *olds)


def adamw_rows(layer, steps, factor, grads, weights, m, v, so_far):
    rows = [w.shape[1] // steps for w in weights]
    columns = [w.shape[2] for w in weights]
    grad_specs = [pl.BlockSpec((r, c), lambda i: (i, 0)) for r, c in zip(rows, columns, strict=True)]
    specs = [pl.BlockSpec((1, r, c), lambda i: (layer, i, 0)) for r, c in zip(rows, columns, strict=True)]
    return adamw_call(whole_kernel, (steps,), (), grads, grad_specs, specs, factor, weights, m, v, so_far)


def adamw_pieces(layer, blocks, pieces, factor, weights, m, v, so_far):
    _, high, width = pieces[0].shape
    rows = high // PIECE_STEPS
    at = jnp.stack([jnp.asarray(b, jnp.int32) for b in blocks])
    per = 2 * PIECE_STEPS

    def piece_spec(k):
        return pl.BlockSpec((3, rows, width), lambda i, at: (0, jnp.clip(i - k * PIECE_STEPS, 0, PIECE_STEPS - 1), 0))

    by_column = pl.BlockSpec((1, rows, width), lambda i, at: (layer, lax.rem(i, per), at[i // per]))
    by_row = pl.BlockSpec((1, width, rows), lambda i, at: (layer, at[i // per], lax.rem(i, per)))
    kernel = functools.partial(pieces_kernel, len(pieces))
    specs = [by_column, by_column, by_row]
    grid = (len(pieces) * PIECE_STEPS,)
    return adamw_call(kernel, grid, (at,), pieces, [piece_spec(k) for k in range(len(pieces))], specs, factor, weights, m, v, so_far)


def solution(mesh):
    n = mesh.shape["dp"]
    to_right = [(i, (i + 1) % n) for i in range(n)]
    to_left = [(i, (i - 1) % n) for i in range(n)]

    def step(x, dy, *arrays):
        weights, m, v = (arrays[i : i + 3] for i in (0, 3, 6))
        me = lax.axis_index("dp")
        top, bottom, common_top, common_bottom, *last, factor = make_gradients(n, x[0], dy[0], *weights)
        rest = (factor, weights, m, v)
        left_top, right_bottom = lax.ppermute(top, "dp", to_right), lax.ppermute(bottom, "dp", to_left)
        left_bottom, right_top = lax.ppermute(bottom, "dp", to_right), lax.ppermute(top, "dp", to_left)
        new = adamw_rows(1, 16, factor, last, weights, m, v, None)
        *new, left_top, right_bottom = lax.optimization_barrier((*new, left_top, right_bottom))
        far_top, far_bottom = lax.ppermute(left_top, "dp", to_right), lax.ppermute(right_bottom, "dp", to_left)
        new = adamw_pieces(0, (me, n), (top, bottom, common_top, common_bottom), *rest, new)
        around = ((me + n - 1) % n, (me + 1) % n)
        new = adamw_pieces(0, around, (left_top, left_bottom, right_top, right_bottom), *rest, new)
        new = adamw_pieces(0, ((me + 2) % n,), (far_top, far_bottom), *rest, new)
        return tuple(new)

    return jax.shard_map(
        step,
        mesh=mesh,
        in_specs=(P(("rep", "dp"), None, None),) * 2 + (P(None, None, None),) * 9,
        out_specs=(P("rep", None, None),) * 9,
        check_vma=False,
    )
```

```python
import functools

import jax
import jax.numpy as jnp
from jax import lax
from jax.experimental import pallas as pl
from jax.experimental.pallas import tpu as pltpu
from jax.sharding import PartitionSpec as P

F32, BF16 = jnp.float32, jnp.bfloat16
ANY, VMEM = pl.ANY, pltpu.VMEM
LANES = 128
WIDE = 512
TILE = 256
ROWS = 512
CHAIN_ROWS = 512
FEW = 128
TURN = 256
PIECE_STEPS = 4
FORWARD_AT = 2
OWN = (640, 512)


def dot(a, b, da=1, db=0):
    return lax.dot_general(a, b, (((da,), (db,)), ((), ())), preferred_element_type=F32)


def aligned(i, size):
    return pl.multiple_of(i * size, size)


def scale_of(wide):
    return lax.rsqrt(jnp.mean(wide**2, -1, keepdims=True) + 1e-6)


def gated(a, dout, w_gate, w_up, w_down):
    gate, up = dot(a, w_gate), dot(a, w_up)
    by_hidden = dot(dout, w_down, 1, 1).astype(BF16).astype(F32)
    s = jax.nn.sigmoid(gate)
    silu = gate * s
    hidden = (silu * up).astype(BF16)
    by_up = (by_hidden * silu).astype(BF16)
    by_gate = (by_hidden * up * (s * (1 + gate * (1 - s)))).astype(BF16)
    return hidden, by_gate, by_up


def gradients_kernel(
    n, count, x, dy, w_gate, w_up, w_down,
    first_top, first_bottom, common_top, common_bottom, last_gate, last_up, last_down, factor, x_all, dy_all, by_all, by_own,
    a_all, d_all, a_t, d_t, chain_gate, chain_up, chain_down, unit_gate, unit_up, unit_down, out_gate, out_up, out_down,
    hidden, by_gate, by_up, total, squares, square,
    chain_sem, unit_sem, out_sem, first_sem, load_sem, send_sem, recv_sem, square_send, square_recv,
):
    tokens, d = x.shape
    ff = w_gate.shape[2]
    half = tokens // 2
    me = lax.axis_index("dp")
    right, left, far = lax.rem(me + 1, n), lax.rem(me + n - 1, n), lax.rem(me + 2, n)

    barrier = pltpu.get_barrier_semaphore()
    for other in (right, left, far):
        pl.semaphore_signal(barrier, inc=1, device_id={"dp": other}, device_id_type=pl.DeviceIdType.MESH)
    pl.semaphore_wait(barrier, n - 1)

    def send(src, dst, sems, to):
        return pltpu.make_async_remote_copy(
            src_ref=src, dst_ref=dst, send_sem=sems[0], recv_sem=sems[1], device_id={"dp": to}, device_id_type=pl.DeviceIdType.MESH
        )

    def ring(number, own, place):
        sems = [(send_sem.at[number + k], recv_sem.at[number + k]) for k in range(4)]
        return (
            (send(own, place(me), sems[0], right), send(own, place(me), sems[1], left)),
            (send(place(left, 0), place(left, 0), sems[2], right), send(place(right, 1), place(right, 1), sems[3], left)),
        )

    def block_of(every):
        return lambda i, k=None: every.at[i] if k is None else every.at[i, pl.ds(k * half, half)]

    def columns_of(full, own):
        def place(i, k=None):
            columns = pl.ds(pl.multiple_of(i * own, LANES), own)
            return full.at[:, columns] if k is None else full.at[pl.ds(k * (d // 2), d // 2), columns]

        return place

    def rows_of(full, own):
        def place(i, k=None):
            if k is None:
                return full.at[pl.ds(pl.multiple_of(i * own, LANES), own)]
            return full.at[pl.ds(pl.multiple_of(i * own + k * (own // 2), own // 2), own // 2)]

        return place

    def start(copies):
        for copy in copies:
            copy.start()

    def wait(copies):
        for copy in copies:
            copy.wait()

    def run(copies):
        start(copies)
        wait(copies)

    dy_ring = ring(0, dy, block_of(dy_all))
    x_ring = ring(4, x, block_of(x_all))
    by_ring = ring(8, by_own, block_of(by_all))
    places = columns_of(last_gate, OWN[1]), columns_of(last_up, OWN[1]), rows_of(last_down, OWN[1])
    last_rings = [ring(12 + 4 * i, place(me), place) for i, place in enumerate(places)]
    last_steps = [[copy for one in last_rings for copy in one[k]] for k in range(2)]

    start(x_ring[0])

    tiles, rest = ff // WIDE, ff % WIDE

    def chain_copies(layer, i, slot, width):
        there, part = pl.ds(pl.multiple_of(i * WIDE, LANES), width), pl.ds(0, width)
        return [
            pltpu.make_async_copy(w_gate.at[layer, :, there], chain_gate.at[slot, :, part], chain_sem.at[slot, 0]),
            pltpu.make_async_copy(w_up.at[layer, :, there], chain_up.at[slot, :, part], chain_sem.at[slot, 1]),
            pltpu.make_async_copy(w_down.at[layer, there], chain_down.at[slot, part], chain_sem.at[slot, 2]),
        ]

    def chain(layer, body, many, between):
        def rows_loop(slot, width):
            def some(r, _):
                body(pl.multiple_of(r * many, many), slot, width)
                return 0

            lax.fori_loop(0, tokens // many, some, 0)

        def tile(i, _):
            slot = lax.rem(i, 2)
            wait(chain_copies(layer, i, slot, WIDE))

            @pl.when(i + 1 < tiles)
            def _():
                start(chain_copies(layer, i + 1, lax.rem(i + 1, 2), WIDE))

            if rest:

                @pl.when(i + 1 == tiles)
                def _():
                    start(chain_copies(layer, tiles, tiles % 2, rest))

            between(i)
            rows_loop(slot, WIDE)
            return 0

        total[...] = jnp.zeros_like(total)
        lax.fori_loop(0, tiles, tile, 0)
        if rest:
            wait(chain_copies(layer, tiles, tiles % 2, rest))
            rows_loop(tiles % 2, rest)

    def forward(r, slot, width):
        rows, units = pl.ds(r, ROWS), pl.ds(0, width)
        a = d_all[at(1, r, ROWS)]
        gate, up = dot(a, chain_gate[slot, :, units]), dot(a, chain_up[slot, :, units])
        total[rows] += dot((jax.nn.silu(gate) * up).astype(BF16), chain_down[slot, units])

    def backward(r, slot, width):
        rows, units = pl.ds(r, CHAIN_ROWS), pl.ds(0, width)
        to_gate, to_up = chain_gate[slot, :, units], chain_up[slot, :, units]
        a, by = a_all[at(me, r, CHAIN_ROWS)], d_all[at(2, r, CHAIN_ROWS)]
        _, gate, up = gated(a, by, to_gate, to_up, chain_down[slot, units])
        total[rows] += dot(gate, to_gate, 1, 1) + dot(up, to_up, 1, 1)

    def each(rows, body, length=tokens):
        def some(r, _):
            body(pl.multiple_of(r * rows, rows))
            return 0

        lax.fori_loop(0, length // rows, some, 0)

    def at(part, r, rows):
        return pl.ds(pl.multiple_of(part * tokens + r, rows), rows)

    def part(i):
        return d_all.at[pl.ds(i * tokens, tokens)]

    def norm_back(r):
        wide = d_all[at(3, r, FEW)].astype(F32)
        scale = scale_of(wide)
        by_a = total[at(0, r, FEW)].astype(BF16).astype(F32)
        by_mean = jnp.sum(by_a * wide, -1, keepdims=True) * -0.5 * (scale * scale * scale)
        by_wide = by_a * scale + wide * (by_mean * (2.0 / d))
        d_all[at(3, r, FEW)] = d_all[at(2, r, FEW)] + by_wide.astype(BF16)

    def take(src, to, sem):
        return [pltpu.make_async_copy(src, part(to), load_sem.at[sem])]

    def pass_x(i):
        @pl.when(i == 4)
        def _():
            wait(x_ring[0])
            start(x_ring[1])
            start(dy_ring[0])

    def sequence(i, _):
        whose = jnp.where(i == 0, me, jnp.where(i == 1, left, jnp.where(i == 2, right, far)))
        states = jnp.where(i == 2, 2, 0)

        @pl.when(i == 0)
        def _():
            wait(take(x, 0, 0))

        @pl.when(i == 1)
        def _():
            wait(take(x_all.at[left], 0, 0))

        @pl.when(i == 2)
        def _():
            wait(take(x_all.at[right], 2, 1))

        @pl.when(i == 3)
        def _():
            wait(take(x_all.at[far], 0, 0))

        def norm_x(r):
            wide = d_all[at(states, r, FEW)].astype(F32)
            d_all[at(1, r, FEW)] = (wide * scale_of(wide)).astype(BF16)

        each(FEW, norm_x)
        chain(0, forward, ROWS, lambda i: None)

        @pl.when(i == 0)
        def _():
            start(chain_copies(1, 0, 0, WIDE))

        @pl.when((i == 1) | (i == 2))
        def _():
            start(chain_copies(0, 0, 0, WIDE))

        @pl.when(i == 2)
        def _():
            wait(x_ring[1])
            start(take(x_all.at[far], 0, 0))
            wait(dy_ring[0])
            start(dy_ring[1])

        def add_layer(r):
            h = d_all[at(states, r, FEW)] + total[at(0, r, FEW)].astype(BF16)
            d_all[at(3, r, FEW)] = h
            wide = h.astype(F32)
            a_all[at(whose, r, FEW)] = (wide * scale_of(wide)).astype(BF16)

        each(FEW, add_layer)

        @pl.when(i == 0)
        def _():
            wait(take(dy, 2, 1))
            chain(1, backward, CHAIN_ROWS, pass_x)
            start(chain_copies(0, 0, 0, WIDE))
            start(take(x_all.at[left], 0, 0))
            each(FEW, norm_back)
            start(take(x_all.at[right], 2, 1))
            run([pltpu.make_async_copy(part(3), by_own, load_sem.at[2])])

        return 0

    start(take(x, 0, 0) + take(dy, 2, 1) + chain_copies(0, 0, 0, WIDE))
    lax.fori_loop(0, n, sequence, 0)

    def load(every, own, there, sem):
        copies = []
        for away in range(n):
            i = lax.rem(me + away, n)
            rows = there.at[pl.ds(pl.multiple_of(i * tokens, tokens), tokens)]
            copies.append(pltpu.make_async_copy(own if away == 0 else every.at[i], rows, load_sem.at[sem + away]))
        return copies

    def turn_states(r):
        a_t[:, pl.ds(r, TURN)] = a_all[pl.ds(r, TURN)].T

    def norm_states(r):
        rows = pl.ds(r, TURN)
        wide = a_all[rows].astype(F32)
        a = (wide * scale_of(wide)).astype(BF16)
        a_all[rows] = a
        a_t[:, rows] = a.T

    def turn_outs(r):
        d_t[:, pl.ds(r, TURN)] = d_all[pl.ds(r, TURN)].T

    squares[...] = jnp.zeros_like(squares)

    def plan(layer):
        mine = OWN[layer] // LANES
        lots = ff // LANES - (n - 1) * mine
        per = TILE // LANES
        count = pl.cdiv(lots, per)

        def units(g):
            g = jnp.minimum(g, lots - 1)
            return pl.ds(pl.multiple_of(jnp.where(g < mine, me * mine + g, (n - 1) * mine + g) * LANES, LANES), LANES)

        def weight_copies(i, slot):
            copies = []
            for p in range(per):
                there, part = units(i * per + p), pl.ds(p * LANES, LANES)
                copies += [
                    pltpu.make_async_copy(w_gate.at[layer, :, there], unit_gate.at[slot, :, part], unit_sem.at[slot, 3 * p]),
                    pltpu.make_async_copy(w_up.at[layer, :, there], unit_up.at[slot, :, part], unit_sem.at[slot, 3 * p + 1]),
                    pltpu.make_async_copy(w_down.at[layer, there], unit_down.at[slot, part], unit_sem.at[slot, 3 * p + 2]),
                ]
            return copies

        return mine, lots, per, count, units, weight_copies

    def first_weights(layer):
        return plan(layer)[-1](0, 0)

    def gradients(layer, targets, between, after):
        mine, lots, per, tiles, units, weight_copies = plan(layer)

        def put(i, slot, act):
            for p in range(per):
                for condition, copies in targets(i * per + p, units(i * per + p), slot, pl.ds(p * LANES, LANES), 4 * p):
                    pl.when(condition & (i * per + p < lots))(functools.partial(act, copies))

        def tile(i, _):
            slot = lax.rem(i, 2)
            wait(weight_copies(i, slot))

            @pl.when(i + 1 < tiles)
            def _():
                start(weight_copies(i + 1, lax.rem(i + 1, 2)))

            between(i)

            def some(r, _):
                rows = pl.ds(pl.multiple_of(r * ROWS, ROWS), ROWS)
                made = gated(a_all[rows], d_all[rows], unit_gate[slot], unit_up[slot], unit_down[slot])
                hidden[rows], by_gate[rows], by_up[rows] = made
                return 0

            lax.fori_loop(0, n * tokens // ROWS, some, 0)

            @pl.when(i >= 1)
            def _():
                put(i - 1, 1 - slot, wait)

            after(i)

            both = jnp.zeros((8, TILE), F32)
            for turned, by, out in ((a_t, by_gate, out_gate), (a_t, by_up, out_up), (d_t, hidden, out_down)):
                g = dot(turned[...], by[...]).astype(BF16)
                if out is out_down and layer:
                    out[slot] = g.T
                elif out is out_down:
                    chain_gate[slot, :, :TILE] = g
                else:
                    out[slot] = g
                wide = g.astype(F32)
                both += jnp.sum((wide * wide).reshape(d // 8, 8, TILE), 0)
            for p in range(per):
                part, g = both[:, p * LANES : (p + 1) * LANES], i * per + p
                squares[0] += jnp.where(g < mine, part, 0.0)
                squares[1] += jnp.where((g >= mine) & (g < lots), part, 0.0)
            put(i, slot, start)
            return 0

        lax.fori_loop(0, tiles, tile, 0)
        put(tiles - 1, (tiles - 1) % 2, wait)

    wait(dy_ring[1])
    start(by_ring[0])
    start(load(dy_all, dy, d_all, n))
    start(first_weights(1))
    each(TURN, turn_states, n * tokens)
    wait(load(dy_all, dy, d_all, n))
    each(TURN, turn_outs, n * tokens)

    def last_targets(g, units, slot, part, sem):
        return [
            (
                g >= 0,
                [
                    pltpu.make_async_copy(out_gate.at[slot, :, part], last_gate.at[:, units], out_sem.at[slot, sem]),
                    pltpu.make_async_copy(out_up.at[slot, :, part], last_up.at[:, units], out_sem.at[slot, sem + 1]),
                    pltpu.make_async_copy(out_down.at[slot, part], last_down.at[units], out_sem.at[slot, sem + 2]),
                ],
            )
        ]

    def forward_on(i):
        @pl.when(i == 3)
        def _():
            wait(by_ring[0])
            start(by_ring[1])

    def load_first(i):
        @pl.when(i == 3)
        def _():
            start(last_steps[0])

        @pl.when(i == plan(1)[3] - 1)
        def _():
            wait(by_ring[1])
            start(load(x_all, x, a_all, 0) + load(by_all, by_own, d_all, n))

    gradients(1, last_targets, forward_on, load_first)
    start(first_weights(0))
    wait(load(x_all, x, a_all, 0) + load(by_all, by_own, d_all, n))
    each(TURN, norm_states, n * tokens)
    each(TURN, turn_outs, n * tokens)

    def first_targets(g, units, slot, part, sem):
        mine = OWN[0] // LANES

        def copies(top, bottom, at):
            columns = pl.ds(pl.multiple_of(at * LANES, LANES), LANES)
            made = []
            for k, to in enumerate((top, bottom)):
                for which, out in enumerate((out_gate, out_up, chain_gate)):
                    some = out.at[slot, pl.ds(k * (d // 2), d // 2), part]
                    made.append(pltpu.make_async_copy(some, to.at[which, :, columns], first_sem.at[slot, sem // 4 * 6 + 3 * k + which]))
            return made

        return [
            (g < mine, copies(first_top, first_bottom, jnp.minimum(g, mine - 1))),
            (g >= mine, copies(common_top, common_bottom, jnp.maximum(g - mine, 0))),
        ]

    def last_on(i):
        @pl.when(i == FORWARD_AT)
        def _():
            wait(last_steps[0])
            start(last_steps[1])

    gradients(0, first_targets, lambda i: None, last_on)

    square[me] = squares[0]
    swaps = [send(square.at[me], square.at[me], (square_send.at[k], square_recv.at[k]), to) for k, to in enumerate((right, left, far))]
    start(swaps)
    wait(swaps)
    wait(last_steps[1])
    every = squares[1]
    for i in range(n):
        every = every + square[i]
    every = jnp.sum(jnp.sum(every, 0, keepdims=True), 1, keepdims=True)
    factor[...] = jnp.broadcast_to(jnp.minimum(1.0, 0.5 * lax.rsqrt(every / count + 1e-30)), factor.shape)


def make_gradients(n, x, dy, w_gate, w_up, w_down):
    tokens, d = x.shape
    layers, _, ff = w_gate.shape
    assert n == 4 and layers == 2
    own, rest = OWN[0], ff - n * OWN[0]
    shape = jax.ShapeDtypeStruct
    every = shape((n, tokens, d), BF16)
    outs = [shape((3, d // 2, own), BF16)] * 2 + [shape((3, d // 2, rest), BF16)] * 2
    outs += [shape((d, ff), BF16)] * 2 + [shape((ff, d), BF16)] + [shape((8, LANES), F32)] + [every] * 3 + [shape((tokens, d), BF16)]
    dma = pltpu.SemaphoreType.DMA
    scratch = [VMEM((n * tokens, d), BF16)] * 2 + [VMEM((d, n * tokens), BF16)] * 2
    scratch += [VMEM((2, d, WIDE), BF16)] * 2 + [VMEM((2, WIDE, d), BF16)]
    scratch += ([VMEM((2, d, TILE), BF16)] * 2 + [VMEM((2, TILE, d), BF16)]) * 2
    scratch += [VMEM((n * tokens, TILE), BF16)] * 3 + [VMEM((tokens, d), F32), VMEM((2, 8, LANES), F32), VMEM((n, 8, LANES), F32)]
    scratch += [dma((2, 3)), dma((2, 6)), dma((2, 8)), dma((2, 12)), dma((2 * n,)), dma((24,)), dma((24,)), dma((3,)), dma((3,))]
    return pl.pallas_call(
        functools.partial(gradients_kernel, n, layers * 3 * d * ff),
        out_shape=outs,
        in_specs=[pl.BlockSpec(memory_space=ANY)] * 5,
        out_specs=[pl.BlockSpec(memory_space=ANY)] * 7 + [pl.BlockSpec(memory_space=VMEM)] + [pl.BlockSpec(memory_space=ANY)] * 4,
        scratch_shapes=scratch,
        compiler_params=pltpu.CompilerParams(collective_id=0, has_side_effects=True, vmem_limit_bytes=67043328),
        cost_estimate=pl.CostEstimate(flops=tokens * d * ff * 2 * 40, bytes_accessed=2**27, transcendentals=0),
        name="gradients",
    )(x, dy, w_gate, w_up, w_down)[:8]


def adamw_update(g, w, m, v, w_out, m_out, v_out):
    m = 0.9 * m[0] + 0.1 * g
    v = 0.95 * v[0] + 0.05 * g * g
    wide = w[0].astype(F32)
    step = m * lax.rsqrt(v + 1e-8) + 0.1 * wide
    w_out[0] = (wide - 0.02 * step).astype(BF16)
    m_out[0] = m
    v_out[0] = v


def whole_kernel(factor, *refs):
    grads, w, m, v = (refs[i : i + 3] for i in (0, 3, 6, 9))
    outs = refs[len(refs) - 9 :]
    for i in range(3):
        adamw_update(grads[i][...].astype(F32) * factor[0:1, 0:1], w[i], m[i], v[i], *outs[i::3])


def pieces_kernel(pieces, at, factor, *refs):
    del at
    w, m, v = (refs[i : i + 3] for i in (pieces, pieces + 3, pieces + 6))
    outs = refs[len(refs) - 9 :]
    piece = pl.program_id(0) // PIECE_STEPS
    g = refs[0][...]
    for k in range(1, pieces):
        g = jnp.where(piece >= k, refs[k][...], g)
    for i in range(3):
        own = g[i].T if i == 2 else g[i]
        adamw_update(own.astype(F32) * factor[0:1, 0:1], w[i], m[i], v[i], *outs[i::3])


def adamw_call(kernel, grid, scalars, grads, grad_specs, specs, factor, weights, m, v, so_far):
    shapes = [jax.ShapeDtypeStruct(a.shape, t) for t in (BF16, F32, F32) for a in weights]
    olds = () if so_far is None else tuple(so_far)
    elements = sum(g.size for g in grads)
    first_old = len(scalars) + 1 + len(grads) + 9
    return pl.pallas_call(
        kernel,
        grid_spec=pltpu.PrefetchScalarGridSpec(
            num_scalar_prefetch=len(scalars),
            grid=grid,
            in_specs=[pl.BlockSpec((8, LANES), lambda *_: (0, 0)), *grad_specs, *(specs * 3)] + [pl.BlockSpec(memory_space=ANY)] * len(olds),
            out_specs=specs * 3,
        ),
        out_shape=shapes,
        input_output_aliases={first_old + i: i for i in range(len(olds))},
        compiler_params=pltpu.CompilerParams(dimension_semantics=("arbitrary",), vmem_limit_bytes=56 * 2**20),
        cost_estimate=pl.CostEstimate(flops=elements * 900, bytes_accessed=elements * 22, transcendentals=elements),
        name="adamw",
    )(*scalars, factor, *grads, *weights, *m, *v, *olds)


def adamw_rows(layer, steps, factor, grads, weights, m, v, so_far):
    rows = [w.shape[1] // steps for w in weights]
    columns = [w.shape[2] for w in weights]
    grad_specs = [pl.BlockSpec((r, c), lambda i: (i, 0)) for r, c in zip(rows, columns, strict=True)]
    specs = [pl.BlockSpec((1, r, c), lambda i: (layer, i, 0)) for r, c in zip(rows, columns, strict=True)]
    return adamw_call(whole_kernel, (steps,), (), grads, grad_specs, specs, factor, weights, m, v, so_far)


def adamw_pieces(layer, blocks, pieces, factor, weights, m, v, so_far):
    _, high, width = pieces[0].shape
    rows = high // PIECE_STEPS
    at = jnp.stack([jnp.asarray(b, jnp.int32) for b in blocks])
    per = 2 * PIECE_STEPS

    def piece_spec(k):
        return pl.BlockSpec((3, rows, width), lambda i, at: (0, jnp.clip(i - k * PIECE_STEPS, 0, PIECE_STEPS - 1), 0))

    by_column = pl.BlockSpec((1, rows, width), lambda i, at: (layer, lax.rem(i, per), at[i // per]))
    by_row = pl.BlockSpec((1, width, rows), lambda i, at: (layer, at[i // per], lax.rem(i, per)))
    kernel = functools.partial(pieces_kernel, len(pieces))
    specs = [by_column, by_column, by_row]
    grid = (len(pieces) * PIECE_STEPS,)
    return adamw_call(kernel, grid, (at,), pieces, [piece_spec(k) for k in range(len(pieces))], specs, factor, weights, m, v, so_far)


def solution(mesh):
    n = mesh.shape["dp"]
    to_right = [(i, (i + 1) % n) for i in range(n)]
    to_left = [(i, (i - 1) % n) for i in range(n)]

    def step(x, dy, *arrays):
        weights, m, v = (arrays[i : i + 3] for i in (0, 3, 6))
        me = lax.axis_index("dp")
        top, bottom, common_top, common_bottom, *last, factor = make_gradients(n, x[0], dy[0], *weights)
        rest = (factor, weights, m, v)
        left_top, right_bottom = lax.ppermute(top, "dp", to_right), lax.ppermute(bottom, "dp", to_left)
        left_bottom, right_top = lax.ppermute(bottom, "dp", to_right), lax.ppermute(top, "dp", to_left)
        new = adamw_rows(1, 16, factor, last, weights, m, v, None)
        *new, left_top, right_bottom = lax.optimization_barrier((*new, left_top, right_bottom))
        far_top, far_bottom = lax.ppermute(left_top, "dp", to_right), lax.ppermute(right_bottom, "dp", to_left)
        new = adamw_pieces(0, (me, n), (top, bottom, common_top, common_bottom), *rest, new)
        around = ((me + n - 1) % n, (me + 1) % n)
        new = adamw_pieces(0, around, (left_top, left_bottom, right_top, right_bottom), *rest, new)
        new = adamw_pieces(0, ((me + 2) % n,), (far_top, far_bottom), *rest, new)
        return tuple(new)

    return jax.shard_map(
        step,
        mesh=mesh,
        in_specs=(P(("rep", "dp"), None, None),) * 2 + (P(None, None, None),) * 9,
        out_specs=(P("rep", None, None),) * 9,
        check_vma=False,
    )
```
